16 devices in a mesh: replica: 2 (over z), data: 8 (over y, x, core).
Axes of the slice: x: 2, y: 2, z: 2, core: 2. Of those that a mesh axis runs over, the one named last changes fastest.
Arguments:
- img_x: bfloat16 [32768, 640], P(('replica', 'data'))
- txt_x: bfloat16 [32768, 768], P(('replica', 'data'))
- w_img: bfloat16 [640, 640], replicated
- w_txt: bfloat16 [768, 640], replicated
- log_temp: float32 [1], replicated
- logit_bias: float32 [1], replicated
Outputs:
- output 1: float32 [1], replicated
- output 2: float32 [1], replicated
- output 3: float32 [1], replicated
- output 4: float32 [640, 640], replicated
- output 5: float32 [768, 640], replicated
All inputs are finite; a program needn't handle non-finite values.
Results may differ from the reference program's by a relative error of at most 0.001.
Values are sent between devices in bfloat16 or wider.
A program may use at most 1 GiB of HBM per device.

```python
import math
import jax
import jax.numpy as jnp
from jax import lax

LOCAL_BATCH = 2048
NUM_DEVICES = 16
IMG_FEAT = 640
TXT_FEAT = 768
EMBED_DIM = 640
LATENT_RANK = 8

GLOBAL_BATCH = LOCAL_BATCH * NUM_DEVICES


def setup_inputs(seed: int = 0) -> dict:
    key_list = jax.random.split(jax.random.key(seed), 12)
    latent = jax.random.normal(key_list[0], (NUM_DEVICES, LOCAL_BATCH, LATENT_RANK), jnp.float32)
    dev_mean = jax.random.normal(key_list[1], (NUM_DEVICES, 1, LATENT_RANK), jnp.float32)
    latent = (latent + 0.8 * dev_mean).reshape(GLOBAL_BATCH, LATENT_RANK)
    mix_img = jax.random.normal(key_list[2], (LATENT_RANK, IMG_FEAT), jnp.float32) * LATENT_RANK ** -0.5
    mix_txt = jax.random.normal(key_list[3], (LATENT_RANK, TXT_FEAT), jnp.float32) * LATENT_RANK ** -0.5
    shared = jax.random.normal(key_list[4], (LATENT_RANK, EMBED_DIM), jnp.float32)
    img_x = 0.7 * (jnp.dot(latent, mix_img) + jax.random.normal(key_list[5], (GLOBAL_BATCH, IMG_FEAT), jnp.float32))
    txt_x = 0.7 * (jnp.dot(latent, mix_txt) + jax.random.normal(key_list[6], (GLOBAL_BATCH, TXT_FEAT), jnp.float32))
    w_img = jnp.dot(mix_img.T, shared) * (LATENT_RANK ** 0.5 / IMG_FEAT) + jax.random.normal(key_list[7], (IMG_FEAT, EMBED_DIM), jnp.float32) * IMG_FEAT ** -0.5
    w_txt = jnp.dot(mix_txt.T, shared) * (LATENT_RANK ** 0.5 / TXT_FEAT) + jax.random.normal(key_list[8], (TXT_FEAT, EMBED_DIM), jnp.float32) * TXT_FEAT ** -0.5
    log_temp = math.log(4.0) + jax.random.uniform(key_list[9], (1,), jnp.float32, -0.3, 0.3)
    logit_bias = -math.log(GLOBAL_BATCH) + jax.random.uniform(key_list[10], (1,), jnp.float32, -0.5, 0.5)
    return {"img_x": img_x.astype(jnp.bfloat16), "txt_x": txt_x.astype(jnp.bfloat16), "w_img": w_img.astype(jnp.bfloat16), "w_txt": w_txt.astype(jnp.bfloat16), "log_temp": log_temp.astype(jnp.float32), "logit_bias": logit_bias.astype(jnp.float32)}


def normalize(raw):
    return raw * lax.rsqrt(jnp.sum(raw * raw, axis=-1, keepdims=True))


def reference(img_x, txt_x, w_img, w_txt, log_temp, logit_bias):
    img_raw = jnp.dot(img_x, w_img, preferred_element_type=jnp.float32)
    txt_raw = jnp.dot(txt_x, w_txt, preferred_element_type=jnp.float32)
    img_unit, img_pull = jax.vjp(normalize, img_raw)
    txt_unit, txt_pull = jax.vjp(normalize, txt_raw)
    img_emb = img_unit.astype(jnp.bfloat16)
    txt_emb = txt_unit.astype(jnp.bfloat16)
    temp_scale = jnp.exp(log_temp[0])
    bias_val = logit_bias[0]
    col_ids = jnp.arange(GLOBAL_BATCH)[None, :]
    row_ids = jnp.arange(LOCAL_BATCH)[:, None]

    def block_step(state_in, block_in):
        d_txt_acc, loss_acc, temp_acc, bias_acc = state_in
        img_blk, blk_idx = block_in
        sim_tile = jnp.dot(img_blk, txt_emb.T, preferred_element_type=jnp.float32)
        logits = temp_scale * sim_tile + bias_val
        labels = jnp.where(col_ids == row_ids + blk_idx * LOCAL_BATCH, 1.0, -1.0)
        loss_part = -jnp.sum(jax.nn.log_sigmoid(labels * logits))
        grad_tile = -labels * jax.nn.sigmoid(-labels * logits) / GLOBAL_BATCH
        grad_b = grad_tile.astype(jnp.bfloat16)
        d_img_blk = temp_scale * jnp.dot(grad_b, txt_emb, preferred_element_type=jnp.float32)
        d_txt_acc = d_txt_acc + jnp.dot(grad_b.T, img_blk, preferred_element_type=jnp.float32)
        new_state = (d_txt_acc, loss_acc + loss_part, temp_acc + jnp.sum(grad_tile * sim_tile), bias_acc + jnp.sum(grad_tile))
        return new_state, d_img_blk

    init_state = (jnp.zeros((GLOBAL_BATCH, EMBED_DIM), jnp.float32), jnp.zeros((), jnp.float32), jnp.zeros((), jnp.float32), jnp.zeros((), jnp.float32))
    img_blocks = img_emb.reshape(NUM_DEVICES, LOCAL_BATCH, EMBED_DIM)
    final_state, d_img_blocks = lax.scan(block_step, init_state, (img_blocks, jnp.arange(NUM_DEVICES)))
    d_txt_acc, loss_sum, temp_sum, bias_sum = final_state
    d_img = d_img_blocks.reshape(GLOBAL_BATCH, EMBED_DIM)
    d_txt = temp_scale * d_txt_acc
    d_img_raw = img_pull(d_img)[0].astype(jnp.bfloat16)
    d_txt_raw = txt_pull(d_txt)[0].astype(jnp.bfloat16)
    d_w_img = jnp.dot(img_x.T, d_img_raw, preferred_element_type=jnp.float32)
    d_w_txt = jnp.dot(txt_x.T, d_txt_raw, preferred_element_type=jnp.float32)
    loss_out = jnp.reshape(loss_sum / GLOBAL_BATCH, (1,))
    d_log_temp = jnp.reshape(temp_scale * temp_sum, (1,))
    d_logit_bias = jnp.reshape(bias_sum, (1,))
    return (loss_out, d_log_temp, d_logit_bias, d_w_img, d_w_txt)
```

```python
import functools

import jax
import jax.numpy as jnp
from jax import lax
from jax.experimental import pallas as pl
from jax.experimental.pallas import tpu as pltpu
from jax.sharding import PartitionSpec as P

F32 = jnp.float32
BF16 = jnp.bfloat16
NN = (((1,), (0,)), ((), ()))
NT = (((1,), (1,)), ((), ()))
LOG2E = 1.4426950408889634
LN2 = 0.6931471805599453
BM, BN, QR = 1024, 512, 16


def dot(a, b, dims=NN):
    return lax.dot_general(a, b, dims, preferred_element_type=F32)


def tile_kernel(diag, has_di, has_dt, *refs):
    refs = list(refs)
    sc_ref, st_in, i_ref, it_ref, ta_ref, tb_ref = refs[:6]
    refs = refs[6:]
    di_in = refs.pop(0) if has_di else None
    dt_in = (refs.pop(0), refs.pop(0)) if has_dt else None
    st_ref, di_ref, dta_ref, dtb_ref, s_buf, g_buf = refs
    step = pl.program_id(0)
    scale, shift = sc_ref[0], sc_ref[1]
    half = ta_ref.shape[1]
    per = half // BN
    chunks = 2 * per

    @pl.when(step == 0)
    def _():
        st_ref[...] = st_in[...]
        for k, out in enumerate((dta_ref, dtb_ref)):
            out[...] = dt_in[k][...] if has_dt else jnp.zeros_like(out)

    def place(c):
        return c // per, pl.ds((c % per) * BN, BN)

    def similarity(c):
        k, cols = place(c)
        s_buf[c % 2] = dot(i_ref[...], (ta_ref, tb_ref)[k][:, cols])

    def pointwise(c):
        over, prod, gsum, gdot = (jnp.zeros((QR, BN), F32) for _ in range(4))
        for r in range(BM // QR):
            rows = pl.ds(r * QR, QR)
            s = s_buf[c % 2, rows, :]
            z = s * scale + shift
            e = jnp.exp2(-jnp.abs(z))
            u = 1.0 + e
            inv = 1.0 / u
            if diag:
                row_id = lax.broadcasted_iota(jnp.int32, (QR, BN), 0) + (r * QR + step * BM)
                col_id = lax.broadcasted_iota(jnp.int32, (QR, BN), 1) + c * BN
                same = row_id == col_id
                z = jnp.where(same, -z, z)
            g = jnp.where(z >= 0, inv, e * inv)
            if diag:
                g = jnp.where(same, -g, g)
            g_buf[c % 2, rows, :] = g.astype(BF16)
            over = over + jnp.maximum(z, 0.0)
            prod = e + prod * u
            gsum = gsum + g
            gdot = gdot + g * s
        st_ref[0] += over
        st_ref[1] += jnp.log1p(prod)
        st_ref[2] += gsum
        st_ref[3] += gdot

    def gradients(c):
        k, cols = place(c)
        g = g_buf[c % 2]
        t_ref, dt_ref = (ta_ref, tb_ref)[k], (dta_ref, dtb_ref)[k]
        dt_ref[:, cols] += dot(it_ref[...], g)
        part = dot(t_ref[:, cols], g, NT)
        if c:
            di_ref[...] += part
        elif has_di:
            di_ref[...] = di_in[...] + part
        else:
            di_ref[...] = part

    for c in range(chunks + 2):
        if c < chunks:
            similarity(c)
        if 1 <= c <= chunks:
            pointwise(c - 1)
        if c >= 2:
            gradients(c - 2)


def tiles(name, sc, st, img, img_t, txt, di=None, dt=None, diag=False):
    rows, dim = img.shape
    half = txt[0].shape[1]
    whole = lambda shape: pl.BlockSpec(shape, lambda g: (0,) * len(shape))
    by_col = pl.BlockSpec((dim, BM), lambda g: (0, g))
    t_spec = whole((dim, half))
    operands = [sc, st, img, img_t, *txt]
    specs = [pl.BlockSpec(memory_space=pltpu.SMEM), whole(st.shape), pl.BlockSpec((BM, dim), lambda g: (g, 0)), by_col, t_spec, t_spec]
    alias = {1: 0}
    if di is not None:
        alias[len(operands)] = 1
        operands.append(di)
        specs.append(by_col)
    if dt is not None:
        for k in range(2):
            alias[len(operands)] = 2 + k
            operands.append(dt[k])
            specs.append(t_spec)
    flops = 6 * rows * 2 * half * dim
    return pl.pallas_call(
        functools.partial(tile_kernel, diag, di is not None, dt is not None),
        name=name,
        grid=(rows // BM,),
        out_shape=(
            jax.ShapeDtypeStruct(st.shape, F32),
            jax.ShapeDtypeStruct((dim, rows), F32),
            jax.ShapeDtypeStruct((dim, half), F32),
            jax.ShapeDtypeStruct((dim, half), F32),
        ),
        in_specs=specs,
        out_specs=(whole(st.shape), by_col, t_spec, t_spec),
        scratch_shapes=[pltpu.VMEM((2, BM, BN), F32), pltpu.VMEM((2, BM, BN), BF16)],
        input_output_aliases=alias,
        cost_estimate=pl.CostEstimate(flops=flops, bytes_accessed=40 * 2**20, transcendentals=0),
        compiler_params=pltpu.CompilerParams(vmem_limit_bytes=60 * 2**20, dimension_semantics=("arbitrary",)),
    )(*operands)


def embed_t(x, w):
    raw = lax.dot_general(w, x, (((0,), (1,)), ((), ())), preferred_element_type=F32)
    inv = lax.rsqrt(jnp.sum(raw * raw, axis=0, keepdims=True))
    return raw * inv, inv


def weight_grad(x, unit, inv, grad):
    raw_grad = (inv * (grad - unit * jnp.sum(unit * grad, axis=0, keepdims=True))).astype(BF16)
    return lax.dot_general(x, raw_grad, (((0,), (1,)), ((), ())), preferred_element_type=F32)


def solution(mesh):
    rep_count, data_count = mesh.shape["replica"], mesh.shape["data"]
    dev_count = rep_count * data_count
    batch_axes = ("replica", "data")
    ring = (0, 1, 3, 2)
    forward = {ring[k]: ring[(k + 1) % 4] for k in range(4)}
    ahead = [(2 * a + k, 2 * b + k) for a, b in forward.items() for k in range(2)]
    back = [(b, a) for a, b in ahead]
    swap_core = [(k, k ^ 1) for k in range(data_count)]
    swap_z = [(0, 1), (1, 0)]

    def local_fn(img_x, txt_x, w_img, w_txt, log_temp, logit_bias):
        total_rows = img_x.shape[0] * dev_count
        go = lambda pair: (lax.ppermute(pair[0], "data", ahead), lax.ppermute(pair[1], "data", back))
        core = lambda x: lax.ppermute(x, "data", swap_core)
        over_z = lambda x: lax.ppermute(x, "replica", swap_z)

        img_unit, img_inv = embed_t(img_x, w_img)
        txt_unit, txt_inv = embed_t(txt_x, w_txt)
        temp_scale = jnp.exp(log_temp[0])
        sc = jnp.stack([temp_scale * LOG2E, logit_bias[0] * LOG2E])
        img_t = img_unit.astype(BF16)
        txt_t = txt_unit.astype(BF16)
        half = txt_t.shape[1] // 2
        b0 = (txt_t[:, :half], txt_t[:, half:])
        b1 = go(b0)
        b2 = go(b1)
        b3 = go(b2)
        peer_t = core(img_t)
        far_t = over_z(img_t)
        far_peer_t = core(far_t)
        img = img_t.T
        peer = peer_t.T
        a0_t = jnp.concatenate([img_t, peer_t], axis=1)
        a1_t = jnp.concatenate([far_t, far_peer_t], axis=1)
        a0 = a0_t.T
        a1 = a1_t.T
        n = img_t.shape[1]

        st = jnp.zeros((4, QR, BN), F32)
        st, di_own, dt0a, dt0b = tiles("own", sc, st, img, img_t, b0, diag=True)
        st, di0, *dt1 = tiles("near1", sc, st, a0, a0_t, b1)
        st, di1, *dt1 = tiles("far1", sc, st, a1, a1_t, b1, dt=dt1)
        dt1 = go(dt1)
        st, di1, *dt2 = tiles("far2", sc, st, a1, a1_t, b2, di=di1)
        st, di1, *dt0 = tiles("far0", sc, st, a1, a1_t, b0, di=di1, dt=(dt0a, dt0b))
        dt2 = (dt1[0] + dt2[0], dt1[1] + dt2[1])
        st, di0, *dt2 = tiles("near2", sc, st, a0, a0_t, b2, di=di0, dt=dt2)
        dt2 = go(dt2)
        st, di1, *dt3 = tiles("far3", sc, st, a1, a1_t, b3, di=di1)
        far_sum = di1[:, :n] + core(di1[:, n:])
        far_sum = over_z(far_sum)
        st, di0, *dt3 = tiles("near3", sc, st, a0, a0_t, b3, di=di0, dt=dt3)
        dt3 = go((dt3[0] + dt2[0], dt3[1] + dt2[1]))
        st, di_peer, *dt0 = tiles("peer0", sc, st, peer, peer_t, b0, dt=dt0)
        d_img = di_own + di0[:, :n] + core(di0[:, n:] + di_peer) + far_sum
        d_txt = jnp.concatenate([dt0[0] + dt3[0], dt0[1] + dt3[1]], axis=1)

        scale = temp_scale / total_rows
        d_w_txt = weight_grad(txt_x, txt_unit, txt_inv, scale * d_txt)
        d_w_img = weight_grad(img_x, img_unit, img_inv, scale * d_img)
        sums = jnp.sum(st, axis=(1, 2))
        loss_sum = sums[0] * LN2 + sums[1]
        totals = jnp.stack([loss_sum / total_rows, temp_scale * sums[3] / total_rows, sums[2] / total_rows])
        totals, d_w_txt = lax.psum((totals, d_w_txt), batch_axes)
        d_w_img = lax.psum(d_w_img, batch_axes)
        return totals[0:1], totals[1:2], totals[2:3], d_w_img, d_w_txt

    batch_spec = P(batch_axes, None)
    return jax.shard_map(local_fn, mesh=mesh, in_specs=(batch_spec, batch_spec, P(), P(), P(), P()), out_specs=(P(), P(), P(), P(), P()), check_vma=False)
```

```python
import functools

import jax
import jax.numpy as jnp
from jax import lax
from jax.experimental import pallas as pl
from jax.experimental.pallas import tpu as pltpu
from jax.sharding import PartitionSpec as P

F32 = jnp.float32
BF16 = jnp.bfloat16
MESH = pl.DeviceIdType.MESH
NN = (((1,), (0,)), ((), ()))
NT = (((1,), (1,)), ((), ()))
LOG2E = 1.4426950408889634
LN2 = 0.6931471805599453
BM, HALF, BN, SN, QR = 1024, 1024, 512, 256, 16
CHUNKS, PER = 2 * HALF // BN, BN // SN
IMG_SEQ = (0, 1, 0, 2, 3, 2, 3, 0, 1, 3, 2, 3, 2, 1, 0, 1)
TXT_SEQ = (0, 1, 1, 1, 1, 2, 2, 2, 2, 3, 3, 0, 0, 3, 3, 0)
STEPS = 2 * len(IMG_SEQ)


def dot(a, b, dims=NN):
    return lax.dot_general(a, b, dims, preferred_element_type=F32)


def entry(seq, u):
    low, high = (sum(v << (2 * k) for k, v in enumerate(part)) for part in (seq[:8], seq[8:]))
    code = low + (u // 8) * (high - low)
    return (code >> (2 * (u % 8))) % 4


def is_first(n):
    return (n < 4) | ((n >= 6) & (n < 10))


def kernel(
    sc_ref, img_ref, txt_ref,
    st_ref, di_ref, dt0_ref, inc_t, inc_core, inc_z, inc_own,
    i_all, it_all, t_all, acc, slots, s_buf, g_buf,
    init_sem, load_sem, store_sem, temp_sem, far_sem, out_sem,
    t_send, t_recv, i_send, i_recv, dt_send, dt_recv, di_send, di_recv,
):
    rep, dat = lax.axis_index("replica"), lax.axis_index("data")
    y, x, core = dat // 4, (dat // 2) % 2, dat % 2
    ahead = (rep, 4 * x + 2 * (1 - y) + core)
    behind = (rep, 4 * (1 - x) + 2 * y + core)
    twin = (rep, 4 * y + 2 * x + (1 - core))
    far = (1 - rep, dat)
    scale, shift = sc_ref[0], sc_ref[1]

    def remote(src, dst, sems, k, to):
        return pltpu.make_async_remote_copy(src_ref=src, dst_ref=dst, send_sem=sems[0].at[k], recv_sem=sems[1].at[k], device_id=to, device_id_type=MESH)

    def txt_hop(s, h):
        src = txt_ref.at[h] if s == 1 else t_all.at[s - 1, h]
        return remote(src, t_all.at[s, h], (t_send, t_recv), 2 * (s - 1) + h, (ahead, behind)[h])

    def img_hop(kind, c):
        src = it_all.at[4 + c] if kind == 2 else img_ref.at[c]
        return remote(src, it_all.at[2 + 2 * kind + c], (i_send, i_recv), 2 * kind + c, (twin, far, twin)[kind])

    def dt_hop(s, h):
        return remote(acc.at[(1, 2, 1)[s], h], inc_t.at[s, h], (dt_send, dt_recv), 2 * s + h, (ahead, behind)[h])

    def di_hop(kind, c):
        src = di_ref.at[(6, 4, 2)[kind] + c]
        return remote(src, (inc_core, inc_z, inc_own)[kind].at[c], (di_send, di_recv), 2 * kind + c, (twin, far, twin)[kind])

    def add_from(dst, src):
        rows = src.shape[0]
        for first in range(0, HALF, 2 * SN):
            copies = [pltpu.make_async_copy(src.at[:, pl.ds(first + p * SN, SN)], s_buf.at[p, pl.ds(0, rows)], temp_sem.at[p]) for p in range(2)]
            for cp in copies:
                cp.start()
            for p, cp in enumerate(copies):
                cp.wait()
                cols = pl.ds(first + p * SN, SN)
                dst[:, cols] += s_buf[p, 0:rows, :]

    def load(chunk, slot):
        return pltpu.make_async_copy(di_ref.at[chunk], slots.at[slot], load_sem.at[slot])

    def store(chunk, slot):
        return pltpu.make_async_copy(slots.at[slot], di_ref.at[chunk], store_sem.at[slot])

    def chunk_of(n):
        return 2 * entry(IMG_SEQ, n // 2) + n % 2

    barrier = pltpu.get_barrier_semaphore()
    for to in (ahead, behind, twin, far):
        pl.semaphore_signal(barrier, inc=1, device_id=to, device_id_type=MESH)
    pl.semaphore_wait(barrier, 4)

    own = [pltpu.make_async_copy(img_ref.at[c], it_all.at[c], init_sem.at[c]) for c in range(2)]
    own += [pltpu.make_async_copy(txt_ref.at[h], t_all.at[0, h], init_sem.at[2 + h]) for h in range(2)]
    for cp in own:
        cp.start()
    for h in range(2):
        txt_hop(1, h).start()
    for c in range(2):
        img_hop(1, c).start()
    for c in range(2):
        img_hop(0, c).start()
    st_ref[...] = jnp.zeros_like(st_ref)
    for cp in own:
        cp.wait()

    def step(n, diag):
        tb = entry(TXT_SEQ, n // 2)
        ab = tb - 2 * (tb // 3)
        chunk, slot, after = chunk_of(n), n % 3, (n + 1) % 3

        if not diag:
            @pl.when(n == 2)
            def _():
                img_hop(0, 0).wait_recv()
                for h in range(2):
                    txt_hop(1, h).wait_recv()
                    txt_hop(2, h).start()

            @pl.when(n == 3)
            def _():
                img_hop(0, 1).wait_recv()

            @pl.when(n == 5)
            def _():
                img_hop(1, 0).wait_recv()
                img_hop(2, 0).start()

            @pl.when(n == 6)
            def _():
                for h in range(2):
                    txt_hop(2, h).wait_recv()
                    txt_hop(3, h).start()

            @pl.when(n == 7)
            def _():
                img_hop(1, 1).wait_recv()
                img_hop(2, 1).start()

            @pl.when(n == 8)
            def _():
                img_hop(2, 0).wait_recv()

            @pl.when(n == 9)
            def _():
                img_hop(2, 1).wait_recv()

            @pl.when(n == 10)
            def _():
                for h in range(2):
                    dt_hop(0, h).start()

            @pl.when(n == 18)
            def _():
                for h in range(2):
                    dt_hop(1, h).start()
                for h in range(2):
                    dt_hop(0, h).wait_send()
                    txt_hop(3, h).wait_recv()

            @pl.when(n == 30)
            def _():
                for h in range(2):
                    dt_hop(2, h).start()

        @pl.when((n == 0) | (n == 2) | (n == 10) | (n == 18))
        def _():
            acc[ab] = jnp.zeros(acc.shape[1:], F32)

        @pl.when(is_first(n))
        def _():
            i_all[chunk] = it_all[chunk].T
            slots[slot] = jnp.zeros(slots.shape[1:], F32)

        @pl.when(jnp.logical_not(is_first(n)))
        def _():
            load(chunk, slot).wait()

        @pl.when((n >= 2) & (n != 26) & (n != 27))
        def _():
            store(chunk_of(n - 2), after).wait()

        @pl.when((n < STEPS - 1) & jnp.logical_not(is_first(n + 1)))
        def _():
            load(chunk_of(n + 1), after).start()

        if not diag:
            for c in range(2):
                @pl.when(n == 24 + c)
                def _():
                    di_hop(0, c).start()

        def similarity(k):
            h, cols = (k * SN) // HALF, pl.ds((k * SN) % HALF, SN)
            s_buf[k % 2] = dot(i_all[chunk], t_all[tb, h, :, cols])

        def pointwise(k):
            over, prod, gsum, gdot = (jnp.zeros((QR, SN), F32) for _ in range(4))
            for r in range(BM // QR):
                rows = pl.ds(r * QR, QR)
                s = s_buf[k % 2, rows, :]
                z = s * scale + shift
                e = jnp.exp2(-jnp.abs(z))
                u = 1.0 + e
                inv = 1.0 / u
                if diag:
                    row_id = lax.broadcasted_iota(jnp.int32, (QR, SN), 0) + (r * QR + n * BM)
                    col_id = lax.broadcasted_iota(jnp.int32, (QR, SN), 1) + k * SN
                    same = row_id == col_id
                    z = jnp.where(same, -z, z)
                g = jnp.where(z >= 0, inv, e * inv)
                if diag:
                    g = jnp.where(same, -g, g)
                g_buf[(k // PER) % 2, rows, pl.ds((k % PER) * SN, SN)] = g.astype(BF16)
                over = over + jnp.maximum(z, 0.0)
                prod = e + prod * u
                gsum = gsum + g
                gdot = gdot + g * s
            st_ref[0] += over
            st_ref[1] += jnp.log1p(prod)
            st_ref[2] += gsum
            st_ref[3] += gdot

        def gradients(c):
            h, cols = (c * BN) // HALF, pl.ds((c * BN) % HALF, BN)
            g = g_buf[c % 2]
            acc[ab, h, :, cols] += dot(it_all[chunk], g)
            slots[slot] += dot(t_all[tb, h, :, cols], g, NT)

        for k in range(CHUNKS * PER + 1 + PER):
            if k < CHUNKS * PER:
                similarity(k)
            if 1 <= k <= CHUNKS * PER:
                pointwise(k - 1)
            if k > PER and (k - 1) % PER == 0:
                gradients((k - 1) // PER - 1)

        if not diag:
            @pl.when(n == 17)
            def _():
                for h in range(2):
                    dt_hop(0, h).wait_recv()
                    add_from(acc.at[2, h], inc_t.at[0, h])

            @pl.when(n == 29)
            def _():
                for h in range(2):
                    dt_hop(1, h).wait_recv()
                    add_from(acc.at[1, h], inc_t.at[1, h])

            for c in range(2):
                @pl.when(n == 24 + c)
                def _():
                    di_hop(0, c).wait_recv()
                    add_from(slots.at[c], inc_core.at[c])
                    to_hbm = pltpu.make_async_copy(slots.at[c], di_ref.at[4 + c], far_sem.at[c])
                    to_hbm.start()
                    to_hbm.wait()
                    di_hop(1, c).start()

        @pl.when((n != 24) & (n != 25))
        def _():
            store(chunk, slot).start()

    lax.fori_loop(0, 2, lambda n, _: step(n, True), None)
    lax.fori_loop(2, STEPS, lambda n, _: step(n, False), None)

    final = [pltpu.make_async_copy(acc.at[0, h], dt0_ref.at[h], out_sem.at[h]) for h in range(2)]
    for c in range(2):
        store(2 + c, (STEPS - 2 + c) % 3).wait()
        di_hop(2, c).start()
    for cp in final:
        cp.start()
    for s in range(1, 4):
        for h in range(2):
            txt_hop(s, h).wait_send()
    for kind in range(3):
        for c in range(2):
            img_hop(kind, c).wait_send()
    for h in range(2):
        dt_hop(1, h).wait_send()
        dt_hop(2, h).wait_send()
    for kind in range(3):
        for c in range(2):
            di_hop(kind, c).wait_send()
    for cp in final:
        cp.wait()
    for h in range(2):
        dt_hop(2, h).wait_recv()
    for kind in (1, 2):
        for c in range(2):
            di_hop(kind, c).wait_recv()


def score(sc, img_t, txt_t):
    dim = img_t.shape[1]
    any_spec = pl.BlockSpec(memory_space=pl.ANY)
    piece = (dim, HALF)
    hbm = lambda *lead: jax.ShapeDtypeStruct((*lead, *piece), F32)
    dma = lambda k: pltpu.SemaphoreType.DMA((k,))
    flops = 6 * STEPS * BM * 2 * HALF * dim
    return pl.pallas_call(
        kernel,
        name="score",
        out_shape=(jax.ShapeDtypeStruct((4, QR, SN), F32), hbm(8), hbm(2), hbm(3, 2), hbm(2), hbm(2), hbm(2)),
        in_specs=[pl.BlockSpec(memory_space=pltpu.SMEM), any_spec, any_spec],
        out_specs=(pl.BlockSpec(memory_space=pltpu.VMEM),) + (any_spec,) * 6,
        scratch_shapes=[
            pltpu.VMEM((8, BM, dim), BF16),
            pltpu.VMEM((8, dim, BM), BF16),
            pltpu.VMEM((4, 2, dim, HALF), BF16),
            pltpu.VMEM((3, 2, dim, HALF), F32),
            pltpu.VMEM((3, dim, BM), F32),
            pltpu.VMEM((2, BM, SN), F32),
            pltpu.VMEM((2, BM, BN), BF16),
            dma(4), dma(3), dma(3), dma(2), dma(2), dma(2),
            dma(6), dma(6), dma(6), dma(6), dma(6), dma(6), dma(6), dma(6),
        ],
        cost_estimate=pl.CostEstimate(flops=flops, bytes_accessed=2**28, transcendentals=0),
        compiler_params=pltpu.CompilerParams(vmem_limit_bytes=67043328, collective_id=0, has_side_effects=True),
    )(sc, img_t, txt_t)


def embed_t(x, w):
    halves = [lax.dot_general(w, x[k * HALF:(k + 1) * HALF], (((0,), (1,)), ((), ())), preferred_element_type=F32) for k in range(2)]
    raw = jnp.stack(halves)
    inv = lax.rsqrt(jnp.sum(raw * raw, axis=1, keepdims=True))
    return raw * inv, inv


def weight_grad(x, unit, inv, grad):
    raw_grad = (inv * (grad - unit * jnp.sum(unit * grad, axis=1, keepdims=True))).astype(BF16)
    parts = [lax.dot_general(x[k * HALF:(k + 1) * HALF], raw_grad[k], (((0,), (1,)), ((), ())), preferred_element_type=F32) for k in range(2)]
    return parts[0] + parts[1]


def solution(mesh):
    dev_count = mesh.shape["replica"] * mesh.shape["data"]
    batch_axes = ("replica", "data")

    def local_fn(img_x, txt_x, w_img, w_txt, log_temp, logit_bias):
        total_rows = img_x.shape[0] * dev_count
        img_unit, img_inv = embed_t(img_x, w_img)
        txt_unit, txt_inv = embed_t(txt_x, w_txt)
        temp_scale = jnp.exp(log_temp[0])
        sc = jnp.stack([temp_scale * LOG2E, logit_bias[0] * LOG2E])
        st, di, dt0, inc_t, _, inc_z, inc_own = score(sc, img_unit.astype(BF16), txt_unit.astype(BF16))
        scale = temp_scale / total_rows
        d_w_txt = weight_grad(txt_x, txt_unit, txt_inv, scale * (dt0 + inc_t[2]))
        d_w_img = weight_grad(img_x, img_unit, img_inv, scale * (di[0:2] + inc_own + inc_z))
        sums = jnp.sum(st, axis=(1, 2))
        loss_sum = sums[0] * LN2 + sums[1]
        totals = jnp.stack([loss_sum / total_rows, temp_scale * sums[3] / total_rows, sums[2] / total_rows])
        totals, d_w_txt, d_w_img = lax.psum((totals, d_w_txt, d_w_img), batch_axes)
        return totals[0:1], totals[1:2], totals[2:3], d_w_img, d_w_txt

    batch_spec = P(batch_axes, None)
    return jax.shard_map(local_fn, mesh=mesh, in_specs=(batch_spec, batch_spec, P(), P(), P(), P()), out_specs=(P(), P(), P(), P(), P()), check_vma=False)
```

```python
import functools

import jax
import jax.numpy as jnp
from jax import lax
from jax.experimental import pallas as pl
from jax.experimental.pallas import tpu as pltpu
from jax.sharding import PartitionSpec as P

F32 = jnp.float32
BF16 = jnp.bfloat16
MESH = pl.DeviceIdType.MESH
NN = (((1,), (0,)), ((), ()))
NT = (((1,), (1,)), ((), ()))
LOG2E = 1.4426950408889634
LN2 = 0.6931471805599453
BM, HALF, BN, SN, QR = 1024, 1024, 512, 256, 16
CHUNKS, PER = 2 * HALF // BN, BN // SN
TAIL = 512
OUT_ROWS, PART = 1536, 96
CHUNK_SEQ = (0, 1, 2, 3, 0, 1, 4, 5, 6, 7, 4, 5, 6, 7, 0, 1, 2, 3, 7, 6, 4, 5, 6, 4, 7, 5, 2, 3, 0, 1, 2, 3)
TXT_SEQ = (0, 0, 1, 1, 1, 1, 1, 1, 1, 1, 2, 2, 2, 2, 2, 2, 2, 2, 3, 3, 3, 3, 0, 0, 0, 0, 3, 3, 3, 3, 0, 0)
STEPS = len(CHUNK_SEQ)


def dot(a, b, dims=NN):
    return lax.dot_general(a, b, dims, preferred_element_type=F32)


def entry(seq, n):
    codes = [sum(v << (3 * k) for k, v in enumerate(seq[first:first + 8])) for first in range(0, STEPS, 8)]
    code = codes[0]
    for k in range(1, len(codes)):
        code = code + jnp.minimum(jnp.maximum(n // 8 - k + 1, 0), 1) * (codes[k] - codes[k - 1])
    return (code >> (3 * (n % 8))) % 8


def is_first(n):
    return (n < 4) | ((n >= 6) & (n < 10))


def kernel(
    sc_ref, img_ref, txt_ref,
    st_ref, di_ref, dt0_ref, inc_t, inc_core, inc_z, inc_own,
    i_all, it_all, t_all, acc, slots, s_buf, g_buf,
    init_sem, load_sem, store_sem, temp_sem, far_sem, out_sem,
    t_send, t_recv, i_send, i_recv, dt_send, dt_recv, di_send, di_recv,
):
    rep, dat = lax.axis_index("replica"), lax.axis_index("data")
    y, x, core = dat // 4, (dat // 2) % 2, dat % 2
    ahead = (rep, 4 * x + 2 * (1 - y) + core)
    behind = (rep, 4 * (1 - x) + 2 * y + core)
    twin = (rep, 4 * y + 2 * x + (1 - core))
    far = (1 - rep, dat)
    across = (rep, 4 * (1 - y) + 2 * (1 - x) + core)
    scale, shift = sc_ref[0], sc_ref[1]

    def remote(src, dst, sems, k, to):
        return pltpu.make_async_remote_copy(src_ref=src, dst_ref=dst, send_sem=sems[0].at[k], recv_sem=sems[1].at[k], device_id=to, device_id_type=MESH)

    def txt_hop(s, h):
        src = txt_ref.at[h] if s == 1 else t_all.at[s - 1, h]
        return remote(src, t_all.at[s, h], (t_send, t_recv), 2 * (s - 1) + h, (ahead, behind)[h])

    def img_hop(kind, c):
        src = it_all.at[4 + c] if kind == 2 else img_ref.at[c]
        return remote(src, it_all.at[2 + 2 * kind + c], (i_send, i_recv), 2 * kind + c, (twin, far, twin)[kind])

    def dt_hop(s, h):
        return remote(acc.at[(1, 2, 1)[s], h], inc_t.at[s, h], (dt_send, dt_recv), 2 * s + h, ((behind, ahead), (across, across), (ahead, behind))[s][h])

    def di_hop(kind, c):
        src = di_ref.at[(6, 4, 2)[kind] + c]
        return remote(src, (inc_core, inc_z, inc_own)[kind].at[c], (di_send, di_recv), 2 * kind + c, (twin, far, twin)[kind])

    def add_from(dst, src):
        rows = src.shape[0]
        for first in range(0, HALF, 2 * SN):
            copies = [pltpu.make_async_copy(src.at[:, pl.ds(first + p * SN, SN)], s_buf.at[p, pl.ds(0, rows)], temp_sem.at[p]) for p in range(2)]
            for cp in copies:
                cp.start()
            for p, cp in enumerate(copies):
                cp.wait()

                def add_rows(i, _):
                    part = pl.ds(i * 64, 64)
                    dst[part, pl.ds(first + p * SN, SN)] += s_buf[p, part, :]

                lax.fori_loop(0, rows // 64, add_rows, None)

    def clear(dst):
        def clear_rows(i, _):
            dst[pl.ds(i * 64, 64), :] = jnp.zeros((64, dst.shape[1]), F32)

        lax.fori_loop(0, dst.shape[0] // 64, clear_rows, None)

    def load(chunk, slot):
        return pltpu.make_async_copy(di_ref.at[chunk], slots.at[slot], load_sem.at[slot])

    def store(chunk, slot):
        return pltpu.make_async_copy(slots.at[slot], di_ref.at[chunk], store_sem.at[slot])

    def chunk_of(n):
        return entry(CHUNK_SEQ, n)

    barrier = pltpu.get_barrier_semaphore()
    for to in (ahead, behind, across, twin, far):
        pl.semaphore_signal(barrier, inc=1, device_id=to, device_id_type=MESH)
    pl.semaphore_wait(barrier, 5)

    own = [pltpu.make_async_copy(img_ref.at[c], it_all.at[c], init_sem.at[c]) for c in range(2)]
    own += [pltpu.make_async_copy(txt_ref.at[h], t_all.at[0, h], init_sem.at[2 + h]) for h in range(2)]
    for cp in own:
        cp.start()
    for h in range(2):
        txt_hop(1, h).start()
    for c in range(2):
        img_hop(1, c).start()
    for c in range(2):
        img_hop(0, c).start()
    st_ref[...] = jnp.zeros_like(st_ref)
    for cp in own:
        cp.wait()

    def arrivals(n):
        @pl.when(n == 2)
        def _():
            img_hop(0, 0).wait_recv()
            for h in range(2):
                txt_hop(1, h).wait_recv()
                txt_hop(2, h).start()

        @pl.when(n == 3)
        def _():
            img_hop(0, 1).wait_recv()

        @pl.when(n == 5)
        def _():
            img_hop(1, 0).wait_recv()
            img_hop(2, 0).start()

        @pl.when(n == 6)
        def _():
            for h in range(2):
                txt_hop(2, h).wait_recv()
                txt_hop(3, h).start()

        @pl.when(n == 7)
        def _():
            img_hop(1, 1).wait_recv()
            img_hop(2, 1).start()

        @pl.when(n == 8)
        def _():
            img_hop(2, 0).wait_recv()

        @pl.when(n == 9)
        def _():
            img_hop(2, 1).wait_recv()

        @pl.when(n == 10)
        def _():
            for h in range(2):
                dt_hop(0, h).start()

        @pl.when(n == 18)
        def _():
            for h in range(2):
                dt_hop(1, h).start()
            for h in range(2):
                dt_hop(0, h).wait_send()
                txt_hop(3, h).wait_recv()

        @pl.when(n == 30)
        def _():
            for h in range(2):
                dt_hop(2, h).start()

    def step(n, diag):
        tb = entry(TXT_SEQ, n)
        ab = tb - 2 * (tb // 3)
        chunk, slot, after = chunk_of(n), n % 3, (n + 1) % 3

        @pl.when((n < 11) | (n == 18) | (n == 30))
        def _():
            if not diag:
                arrivals(n)

            @pl.when((n == 0) | (n == 2) | (n == 10) | (n == 18))
            def _():
                for h in range(2):
                    clear(acc.at[ab, h])

            @pl.when(is_first(n))
            def _():
                def turn(i, _):
                    part = pl.ds(pl.multiple_of(i * 256, 256), 256)
                    i_all[chunk, part, :] = it_all[chunk, :, part].T

                lax.fori_loop(0, BM // 256, turn, None)
                clear(slots.at[slot])

        @pl.when(jnp.logical_not(is_first(n)))
        def _():
            load(chunk, slot).wait()

        @pl.when((n >= 2) & (n != 24) & (n != 25) & (n != 26) & (n != 27))
        def _():
            store(chunk_of(n - 2), after).wait()

        @pl.when((n < STEPS - 1) & jnp.logical_not(is_first(n + 1)))
        def _():
            load(chunk_of(n + 1), after).start()

        if not diag:
            @pl.when((n == 23) | (n == 25))
            def _():
                store(chunk_of(n - 1), (n - 1) % 3).wait()
                di_hop(0, (n - 23) // 2).start()

        def similarity(k):
            h, cols = (k * SN) // HALF, pl.ds((k * SN) % HALF, SN)
            s_buf[k % 2] = dot(i_all[chunk], t_all[tb, h, :, cols])

        def pointwise(k):
            over, prod, gsum, gdot = (jnp.zeros((QR, SN), F32) for _ in range(4))
            for r in range(BM // QR):
                rows = pl.ds(r * QR, QR)
                s = s_buf[k % 2, rows, :]
                z = s * scale + shift
                e = jnp.exp2(-jnp.abs(z))
                u = 1.0 + e
                inv = 1.0 / u
                if diag:
                    row_id = lax.broadcasted_iota(jnp.int32, (QR, SN), 0) + (r * QR + n * BM)
                    col_id = lax.broadcasted_iota(jnp.int32, (QR, SN), 1) + k * SN
                    same = row_id == col_id
                    z = jnp.where(same, -z, z)
                g = jnp.where(z >= 0, inv, e * inv)
                if diag:
                    g = jnp.where(same, -g, g)
                g_buf[(k // PER) % 2, rows, pl.ds((k % PER) * SN, SN)] = g.astype(BF16)
                over = over + jnp.maximum(z, 0.0)
                prod = e + prod * u
                gsum = gsum + g
                gdot = gdot + g * s
            st_ref[0] += over
            st_ref[1] += jnp.log1p(prod)
            st_ref[2] += gsum
            st_ref[3] += gdot

        def gradients(c):
            h, cols = (c * BN) // HALF, pl.ds((c * BN) % HALF, BN)
            g = g_buf[c % 2]
            acc[ab, h, :, cols] += dot(it_all[chunk], g)
            slots[slot] += dot(t_all[tb, h, :, cols], g, NT)

        for k in range(CHUNKS * PER + 1 + PER):
            if k < CHUNKS * PER:
                similarity(k)
            if 1 <= k <= CHUNKS * PER:
                pointwise(k - 1)
            if k > PER and (k - 1) % PER == 0:
                gradients((k - 1) // PER - 1)

        if not diag:
            @pl.when((n == 23) | (n == 25))
            def _():
                c = (n - 23) // 2
                di_hop(0, c).wait_recv()
                add_from(slots.at[slot], inc_core.at[c])
                to_hbm = pltpu.make_async_copy(slots.at[slot], di_ref.at[4 + c], far_sem.at[c])
                to_hbm.start()
                to_hbm.wait()
                di_hop(1, c).start()

        @pl.when((n != 23) & (n != 25))
        def _():
            store(chunk, slot).start()

    lax.fori_loop(0, 2, lambda n, _: step(n, True), None)
    lax.fori_loop(2, STEPS, lambda n, _: step(n, False), None)

    final = [pltpu.make_async_copy(acc.at[0, h], dt0_ref.at[h], out_sem.at[h]) for h in range(2)]
    for c in range(2):
        store(2 + c, (STEPS - 2 + c) % 3).wait()
        di_hop(2, c).start()
    for cp in final:
        cp.start()
    for s in range(1, 4):
        for h in range(2):
            txt_hop(s, h).wait_send()
    for kind in range(3):
        for c in range(2):
            img_hop(kind, c).wait_send()
    for h in range(2):
        dt_hop(1, h).wait_send()
        dt_hop(2, h).wait_send()
    for kind in range(3):
        for c in range(2):
            di_hop(kind, c).wait_send()
    for cp in final:
        cp.wait()
    for s in range(3):
        for h in range(2):
            dt_hop(s, h).wait_recv()
    for kind in (1, 2):
        for c in range(2):
            di_hop(kind, c).wait_recv()


def score(sc, img_t, txt_t):
    dim = img_t.shape[1]
    any_spec = pl.BlockSpec(memory_space=pl.ANY)
    piece = (dim, HALF)
    hbm = lambda *lead: jax.ShapeDtypeStruct((*lead, *piece), F32)
    dma = lambda k: pltpu.SemaphoreType.DMA((k,))
    flops = 6 * STEPS * BM * 2 * HALF * dim
    return pl.pallas_call(
        kernel,
        name="score",
        out_shape=(jax.ShapeDtypeStruct((4, QR, SN), F32), hbm(8), hbm(2), hbm(3, 2), hbm(2), hbm(2), hbm(2)),
        in_specs=[pl.BlockSpec(memory_space=pltpu.SMEM), any_spec, any_spec],
        out_specs=(pl.BlockSpec(memory_space=pltpu.VMEM),) + (any_spec,) * 6,
        scratch_shapes=[
            pltpu.VMEM((8, BM, dim), BF16),
            pltpu.VMEM((8, dim, BM), BF16),
            pltpu.VMEM((4, 2, dim, HALF), BF16),
            pltpu.VMEM((3, 2, dim, HALF), F32),
            pltpu.VMEM((3, dim, BM), F32),
            pltpu.VMEM((2, BM, SN), F32),
            pltpu.VMEM((2, BM, BN), BF16),
            dma(4), dma(3), dma(3), dma(2), dma(2), dma(2),
            dma(6), dma(6), dma(6), dma(6), dma(6), dma(6), dma(6), dma(6),
        ],
        cost_estimate=pl.CostEstimate(flops=flops, bytes_accessed=2**28, transcendentals=0),
        compiler_params=pltpu.CompilerParams(vmem_limit_bytes=67043328, collective_id=0, has_side_effects=True),
    )(sc, img_t, txt_t)


def embed_t(x, w):
    halves = [lax.dot_general(w, x[k * HALF:(k + 1) * HALF], (((0,), (1,)), ((), ())), preferred_element_type=F32) for k in range(2)]
    raw = jnp.stack(halves)
    inv = lax.rsqrt(jnp.sum(raw * raw, axis=1, keepdims=True))
    return raw, (raw * inv).astype(BF16)


def tail_kernel(img_sc, txt_sc, st_ref, *refs):
    *ins, out_ref, img_acc, txt_acc = refs
    sums, raws, xs = ins[:3], ins[3], ins[4]
    txt_sums, txt_raw, txt_x = ins[5:9], ins[9], ins[10]
    g = pl.program_id(0)
    dim, img_rows = out_ref.shape[1], xs.shape[1]

    def add_rows(factor, parts, raw_ref, x_ref, acc, start):
        total = parts[0][...].reshape(dim, TAIL)
        for part in parts[1:]:
            total = total + part[...].reshape(dim, TAIL)
        grad = factor[0] * total
        raw = raw_ref[0]
        inv = lax.rsqrt(jnp.sum(raw * raw, axis=0, keepdims=True))
        unit = raw * inv
        raw_grad = inv * (grad - unit * jnp.sum(unit * grad, axis=0, keepdims=True))
        part = dot(raw_grad.astype(BF16), x_ref[...])

        @pl.when(g == start)
        def _():
            acc[...] = part

        @pl.when(g > start)
        def _():
            acc[...] += part

    @pl.when(g < 4)
    def _():
        add_rows(img_sc, sums, raws, xs, img_acc, 0)

    @pl.when(g >= 4)
    def _():
        add_rows(txt_sc, txt_sums, txt_raw, txt_x, txt_acc, 4)

    @pl.when(g == 4)
    def _():
        out_ref[0:img_rows, :] = img_acc[...].T

    @pl.when(g == 7)
    def _():
        last = img_rows + txt_acc.shape[1]
        out_ref[img_rows:last, :] = txt_acc[...].T
        total_rows = txt_sc[1]
        loss = (jnp.sum(st_ref[0]) * LN2 + jnp.sum(st_ref[1])) / total_rows
        d_temp = txt_sc[0] * jnp.sum(st_ref[3])
        d_bias = jnp.sum(st_ref[2]) / total_rows
        row = lax.broadcasted_iota(jnp.int32, (OUT_ROWS - last, dim), 0)
        out_ref[last:OUT_ROWS, :] = jnp.where(row == 0, loss, jnp.where(row == 1, d_temp, d_bias))


def tail(sc, st, di, inc_own, inc_z, img_raw, img_x, dt0, inc_t, txt_raw, txt_x):
    dim = img_raw.shape[1]
    img_f, txt_f = img_x.shape[1], txt_x.shape[1]
    img_g = lambda g: jnp.minimum(g, 3)
    txt_g = lambda g: jnp.maximum(g - 4, 0)
    block = lambda at: pl.BlockSpec((1, dim, TAIL), lambda g: (at(g) // 2, 0, at(g) % 2))
    rows = lambda at, f: pl.BlockSpec((TAIL, f), lambda g: (at(g), 0))
    hop = lambda s: pl.BlockSpec((1, 1, dim, TAIL), lambda g: (s, txt_g(g) // 2, 0, txt_g(g) % 2))
    smem = pl.BlockSpec(memory_space=pltpu.SMEM)
    out_rows = OUT_ROWS
    return pl.pallas_call(
        tail_kernel,
        name="tail",
        grid=(8,),
        out_shape=jax.ShapeDtypeStruct((out_rows, dim), F32),
        in_specs=[smem, smem, pl.BlockSpec(st.shape, lambda g: (0, 0, 0)), block(img_g), block(img_g), block(img_g), block(img_g), rows(img_g, img_f),
                  block(txt_g), hop(0), hop(1), hop(2), block(txt_g), rows(txt_g, txt_f)],
        out_specs=pl.BlockSpec((out_rows, dim), lambda g: (0, 0)),
        scratch_shapes=[pltpu.VMEM((dim, img_f), F32), pltpu.VMEM((dim, txt_f), F32)],
        compiler_params=pltpu.CompilerParams(vmem_limit_bytes=60 * 2**20, dimension_semantics=("arbitrary",)),
    )(sc, sc, st, di, inc_own, inc_z, img_raw, img_x, dt0, inc_t, inc_t, inc_t, txt_raw, txt_x)


def reduce_kernel(x_ref, img_ref, txt_ref, tot_ref, from_twin, part, got, res, t_send, t_recv, p_send, p_recv, g_send, g_recv, f_send, f_recv, out_sem):
    rep, dat = lax.axis_index("replica"), lax.axis_index("data")
    y, x, core = dat // 4, (dat // 2) % 2, dat % 2

    def flip(bit, on):
        return 1 - bit if on else bit

    def chip(q):
        return flip(rep, q & 4), flip(y, q & 2), flip(x, q & 1)

    def device(q):
        cz, cy, cx = chip(q)
        return (cz, 4 * cy + 2 * cx + core)

    def rows(c, k):
        return pl.ds((2 * c + k) * PART, PART)

    def number(q):
        cz, cy, cx = chip(q)
        return 4 * cz + 2 * cy + cx

    twin = (rep, 4 * y + 2 * x + (1 - core))

    def remote(src, dst, sems, k, to):
        return pltpu.make_async_remote_copy(src_ref=src, dst_ref=dst, send_sem=sems[0].at[k], recv_sem=sems[1].at[k], device_id=to, device_id_type=MESH)

    barrier = pltpu.get_barrier_semaphore()
    for to in [twin] + [device(q) for q in range(1, 8)]:
        pl.semaphore_signal(barrier, inc=1, device_id=to, device_id_type=MESH)
    pl.semaphore_wait(barrier, 8)

    halves = [remote(x_ref.at[rows(c, 1 - core)], from_twin.at[c], (t_send, t_recv), c, twin) for c in range(8)]
    for cp in halves:
        cp.start()
    for c, cp in enumerate(halves):
        cp.wait_recv()
        part[c] = x_ref[rows(c, core), :] + from_twin[c]
    parts = [remote(part.at[number(q)], got.at[q - 1], (p_send, p_recv), q - 1, device(q)) for q in range(1, 8)]
    for cp in parts:
        cp.start()
    total = part[number(0)]
    for q, cp in enumerate(parts):
        cp.wait_recv()
        total = total + got[q]
    mine = rows(number(0), core)
    res[mine, :] = total
    spread = [remote(res.at[mine], res.at[mine], (g_send, g_recv), q - 1, device(q)) for q in range(1, 8)]
    for cp in spread:
        cp.start()
    forward = [remote(res.at[rows(number(q), core)], res.at[rows(number(q), core)], (f_send, f_recv), q, twin) for q in range(8)]
    forward[0].start()
    for q in range(1, 8):
        arrived = res.at[rows(number(q), core)]
        remote(arrived, arrived, (g_send, g_recv), q - 1, device(q)).wait_recv()
        forward[q].start()
    for q in range(8):
        other = res.at[rows(number(q), 1 - core)]
        remote(other, other, (f_send, f_recv), q, twin).wait_recv()
    first, last = img_ref.shape[0], img_ref.shape[0] + txt_ref.shape[0]
    spans = ((img_ref, 0, first), (txt_ref, first, last), (tot_ref, last, last + 8))
    outs = [pltpu.make_async_copy(res.at[pl.ds(lo, hi - lo)], ref, out_sem.at[k]) for k, (ref, lo, hi) in enumerate(spans)]
    for cp in outs:
        cp.start()
    for cp in halves + parts + spread + forward:
        cp.wait_send()
    for cp in outs:
        cp.wait()


def reduce_all(x, img_f, txt_f):
    dim = x.shape[1]
    any_spec = pl.BlockSpec(memory_space=pl.ANY)
    dma = lambda k: pltpu.SemaphoreType.DMA((k,))
    return pl.pallas_call(
        reduce_kernel,
        name="reduce",
        out_shape=tuple(jax.ShapeDtypeStruct((k, dim), F32) for k in (img_f, txt_f, 8)),
        in_specs=[pl.BlockSpec(memory_space=pltpu.VMEM)],
        out_specs=(any_spec,) * 3,
        scratch_shapes=[
            pltpu.VMEM((8, PART, dim), F32),
            pltpu.VMEM((8, PART, dim), F32),
            pltpu.VMEM((7, PART, dim), F32),
            pltpu.VMEM((OUT_ROWS, dim), F32),
            dma(8), dma(8), dma(7), dma(7), dma(7), dma(7), dma(8), dma(8), dma(3),
        ],
        compiler_params=pltpu.CompilerParams(vmem_limit_bytes=40 * 2**20, collective_id=1, has_side_effects=True),
    )(x)


def solution(mesh):
    dev_count = mesh.shape["replica"] * mesh.shape["data"]
    batch_axes = ("replica", "data")

    def local_fn(img_x, txt_x, w_img, w_txt, log_temp, logit_bias):
        total_rows = img_x.shape[0] * dev_count
        img_raw, img_t = embed_t(img_x, w_img)
        txt_raw, txt_t = embed_t(txt_x, w_txt)
        temp_scale = jnp.exp(log_temp[0])
        sc = jnp.stack([temp_scale * LOG2E, logit_bias[0] * LOG2E])
        st, di, dt0, inc_t, _, inc_z, inc_own = score(sc, img_t, txt_t)
        factors = jnp.stack([temp_scale / total_rows, jnp.float32(total_rows)])
        grads = tail(factors, st, di, inc_own, inc_z, img_raw, img_x, dt0, inc_t, txt_raw, txt_x)
        d_w_img, d_w_txt, totals = reduce_all(grads, img_x.shape[1], txt_x.shape[1])
        return totals[0, 0:1], totals[1, 0:1], totals[2, 0:1], d_w_img, d_w_txt

    batch_spec = P(batch_axes, None)
    return jax.shard_map(local_fn, mesh=mesh, in_specs=(batch_spec, batch_spec, P(), P(), P(), P()), out_specs=(P(), P(), P(), P(), P()), check_vma=False)
```

```python
import functools

import jax
import jax.numpy as jnp
from jax import lax
from jax.experimental import pallas as pl
from jax.experimental.pallas import tpu as pltpu
from jax.sharding import PartitionSpec as P

F32 = jnp.float32
BF16 = jnp.bfloat16
MESH = pl.DeviceIdType.MESH
NN = (((1,), (0,)), ((), ()))
NT = (((1,), (1,)), ((), ()))
LOG2E = 1.4426950408889634
LN2 = 0.6931471805599453
BM, HALF, BN, SN, QR = 1024, 1024, 512, 256, 16
CHUNKS, PER = 2 * HALF // BN, BN // SN
TAIL = 512
OUT_ROWS, PART = 1536, 96
CHUNK_SEQ = (0, 1, 2, 3, 0, 1, 4, 5, 6, 7, 4, 5, 6, 7, 0, 1, 2, 3, 7, 6, 4, 5, 6, 4, 7, 5, 2, 3, 0, 1, 2, 3)
TXT_SEQ = (0, 0, 1, 1, 1, 1, 1, 1, 1, 1, 2, 2, 2, 2, 2, 2, 2, 2, 3, 3, 3, 3, 0, 0, 0, 0, 3, 3, 3, 3, 0, 0)
STEPS = len(CHUNK_SEQ)


def dot(a, b, dims=NN):
    return lax.dot_general(a, b, dims, preferred_element_type=F32)


def entry(seq, n):
    codes = [sum(v << (3 * k) for k, v in enumerate(seq[first:first + 8])) for first in range(0, STEPS, 8)]
    code = codes[0]
    for k in range(1, len(codes)):
        code = code + jnp.minimum(jnp.maximum(n // 8 - k + 1, 0), 1) * (codes[k] - codes[k - 1])
    return (code >> (3 * (n % 8))) % 8


def is_first(n):
    return (n < 4) | ((n >= 6) & (n < 10))


def kernel(
    sc_ref, img_ref, txt_ref,
    st_ref, di_ref, dt0_ref, inc_t, inc_core, inc_z, inc_own,
    i_all, it_all, t_all, acc, slots, s_buf, g_buf,
    init_sem, load_sem, store_sem, temp_sem, far_sem, out_sem,
    t_send, t_recv, i_send, i_recv, dt_send, dt_recv, di_send, di_recv,
):
    rep, dat = lax.axis_index("replica"), lax.axis_index("data")
    y, x, core = dat // 4, (dat // 2) % 2, dat % 2
    ahead = (rep, 4 * x + 2 * (1 - y) + core)
    behind = (rep, 4 * (1 - x) + 2 * y + core)
    twin = (rep, 4 * y + 2 * x + (1 - core))
    far = (1 - rep, dat)
    across = (rep, 4 * (1 - y) + 2 * (1 - x) + core)
    scale, shift = sc_ref[0], sc_ref[1]

    def remote(src, dst, sems, k, to):
        return pltpu.make_async_remote_copy(src_ref=src, dst_ref=dst, send_sem=sems[0].at[k], recv_sem=sems[1].at[k], device_id=to, device_id_type=MESH)

    def txt_hop(s, h):
        src = txt_ref.at[:, pl.ds(h * HALF, HALF)] if s == 1 else t_all.at[s - 1, h]
        return remote(src, t_all.at[s, h], (t_send, t_recv), 2 * (s - 1) + h, (ahead, behind)[h])

    def img_hop(kind, c):
        src = it_all.at[4 + c] if kind == 2 else img_ref.at[:, pl.ds(c * BM, BM)]
        return remote(src, it_all.at[2 + 2 * kind + c], (i_send, i_recv), 2 * kind + c, (twin, far, twin)[kind])

    def dt_hop(s, h):
        return remote(acc.at[(1, 2, 1)[s], h], inc_t.at[s, h], (dt_send, dt_recv), 2 * s + h, ((behind, ahead), (across, across), (ahead, behind))[s][h])

    def di_hop(kind, c):
        src = di_ref.at[(6, 4, 2)[kind] + c]
        return remote(src, (inc_core, inc_z, inc_own)[kind].at[c], (di_send, di_recv), 2 * kind + c, (twin, far, twin)[kind])

    def add_from(dst, src):
        rows = src.shape[0]
        for first in range(0, HALF, 2 * SN):
            copies = [pltpu.make_async_copy(src.at[:, pl.ds(first + p * SN, SN)], s_buf.at[p, pl.ds(0, rows)], temp_sem.at[p]) for p in range(2)]
            for cp in copies:
                cp.start()
            for p, cp in enumerate(copies):
                cp.wait()

                def add_rows(i, _):
                    part = pl.ds(i * 64, 64)
                    dst[part, pl.ds(first + p * SN, SN)] += s_buf[p, part, :]

                lax.fori_loop(0, rows // 64, add_rows, None)

    def clear(dst):
        def clear_rows(i, _):
            dst[pl.ds(i * 64, 64), :] = jnp.zeros((64, dst.shape[1]), F32)

        lax.fori_loop(0, dst.shape[0] // 64, clear_rows, None)

    def load(chunk, slot):
        return pltpu.make_async_copy(di_ref.at[chunk], slots.at[slot], load_sem.at[slot])

    def store(chunk, slot):
        return pltpu.make_async_copy(slots.at[slot], di_ref.at[chunk], store_sem.at[slot])

    def chunk_of(n):
        return entry(CHUNK_SEQ, n)

    barrier = pltpu.get_barrier_semaphore()
    for to in (ahead, behind, across, twin, far):
        pl.semaphore_signal(barrier, inc=1, device_id=to, device_id_type=MESH)
    pl.semaphore_wait(barrier, 5)

    own = [pltpu.make_async_copy(img_ref.at[:, pl.ds(c * BM, BM)], it_all.at[c], init_sem.at[c]) for c in range(2)]
    own += [pltpu.make_async_copy(txt_ref.at[:, pl.ds(h * HALF, HALF)], t_all.at[0, h], init_sem.at[2 + h]) for h in range(2)]
    for cp in own:
        cp.start()
    for h in range(2):
        txt_hop(1, h).start()
    for c in range(2):
        img_hop(1, c).start()
    for c in range(2):
        img_hop(0, c).start()
    st_ref[...] = jnp.zeros_like(st_ref)
    for cp in own:
        cp.wait()

    def arrivals(n):
        @pl.when(n == 2)
        def _():
            img_hop(0, 0).wait_recv()
            for h in range(2):
                txt_hop(1, h).wait_recv()
                txt_hop(2, h).start()

        @pl.when(n == 3)
        def _():
            img_hop(0, 1).wait_recv()

        @pl.when(n == 5)
        def _():
            img_hop(1, 0).wait_recv()
            img_hop(2, 0).start()

        @pl.when(n == 6)
        def _():
            for h in range(2):
                txt_hop(2, h).wait_recv()
                txt_hop(3, h).start()

        @pl.when(n == 7)
        def _():
            img_hop(1, 1).wait_recv()
            img_hop(2, 1).start()

        @pl.when(n == 8)
        def _():
            img_hop(2, 0).wait_recv()

        @pl.when(n == 9)
        def _():
            img_hop(2, 1).wait_recv()

        @pl.when(n == 10)
        def _():
            for h in range(2):
                dt_hop(0, h).start()

        @pl.when(n == 18)
        def _():
            for h in range(2):
                dt_hop(1, h).start()
            for h in range(2):
                dt_hop(0, h).wait_send()
                txt_hop(3, h).wait_recv()

        @pl.when(n == 30)
        def _():
            for h in range(2):
                dt_hop(2, h).start()

    def step(n, diag):
        tb = entry(TXT_SEQ, n)
        ab = tb - 2 * (tb // 3)
        chunk, slot, after = chunk_of(n), n % 3, (n + 1) % 3

        @pl.when((n < 11) | (n == 18) | (n == 30))
        def _():
            if not diag:
                arrivals(n)

            @pl.when((n == 0) | (n == 2) | (n == 10) | (n == 18))
            def _():
                for h in range(2):
                    clear(acc.at[ab, h])

            @pl.when(is_first(n))
            def _():
                def turn(i, _):
                    part = pl.ds(pl.multiple_of(i * 256, 256), 256)
                    i_all[chunk, part, :] = it_all[chunk, :, part].T

                lax.fori_loop(0, BM // 256, turn, None)
                clear(slots.at[slot])

        @pl.when(jnp.logical_not(is_first(n)))
        def _():
            load(chunk, slot).wait()

        @pl.when((n >= 2) & (n != 24) & (n != 25) & (n != 26) & (n != 27))
        def _():
            store(chunk_of(n - 2), after).wait()

        @pl.when((n < STEPS - 1) & jnp.logical_not(is_first(n + 1)))
        def _():
            load(chunk_of(n + 1), after).start()

        if not diag:
            @pl.when((n == 23) | (n == 25))
            def _():
                store(chunk_of(n - 1), (n - 1) % 3).wait()
                di_hop(0, (n - 23) // 2).start()

        def similarity(k):
            h, cols = (k * SN) // HALF, pl.ds((k * SN) % HALF, SN)
            s_buf[k % 2] = dot(i_all[chunk], t_all[tb, h, :, cols])

        def pointwise(k):
            over, prod, gsum, gdot = (jnp.zeros((QR, SN), F32) for _ in range(4))
            for r in range(BM // QR):
                rows = pl.ds(r * QR, QR)
                s = s_buf[k % 2, rows, :]
                z = s * scale + shift
                e = jnp.exp2(-jnp.abs(z))
                u = 1.0 + e
                inv = 1.0 / u
                if diag:
                    row_id = lax.broadcasted_iota(jnp.int32, (QR, SN), 0) + (r * QR + n * BM)
                    col_id = lax.broadcasted_iota(jnp.int32, (QR, SN), 1) + k * SN
                    same = row_id == col_id
                    z = jnp.where(same, -z, z)
                g = jnp.where(z >= 0, inv, e * inv)
                if diag:
                    g = jnp.where(same, -g, g)
                g_buf[(k // PER) % 2, rows, pl.ds((k % PER) * SN, SN)] = g.astype(BF16)
                over = over + jnp.maximum(z, 0.0)
                prod = e + prod * u
                gsum = gsum + g
                gdot = gdot + g * s
            st_ref[0] += over
            st_ref[1] += jnp.log1p(prod)
            st_ref[2] += gsum
            st_ref[3] += gdot

        def gradients(c):
            h, cols = (c * BN) // HALF, pl.ds((c * BN) % HALF, BN)
            g = g_buf[c % 2]
            acc[ab, h, :, cols] += dot(it_all[chunk], g)
            slots[slot] += dot(t_all[tb, h, :, cols], g, NT)

        for k in range(CHUNKS * PER + 1 + PER):
            if k < CHUNKS * PER:
                similarity(k)
            if 1 <= k <= CHUNKS * PER:
                pointwise(k - 1)
            if k > PER and (k - 1) % PER == 0:
                gradients((k - 1) // PER - 1)

        if not diag:
            @pl.when((n == 23) | (n == 25))
            def _():
                c = (n - 23) // 2
                di_hop(0, c).wait_recv()
                add_from(slots.at[slot], inc_core.at[c])
                to_hbm = pltpu.make_async_copy(slots.at[slot], di_ref.at[4 + c], far_sem.at[c])
                to_hbm.start()
                to_hbm.wait()
                di_hop(1, c).start()

        @pl.when((n != 23) & (n != 25))
        def _():
            store(chunk, slot).start()

    lax.fori_loop(0, 2, lambda n, _: step(n, True), None)
    lax.fori_loop(2, STEPS, lambda n, _: step(n, False), None)

    final = [pltpu.make_async_copy(acc.at[0, h], dt0_ref.at[h], out_sem.at[h]) for h in range(2)]
    for c in range(2):
        store(2 + c, (STEPS - 2 + c) % 3).wait()
        di_hop(2, c).start()
    for cp in final:
        cp.start()
    for s in range(1, 4):
        for h in range(2):
            txt_hop(s, h).wait_send()
    for kind in range(3):
        for c in range(2):
            img_hop(kind, c).wait_send()
    for h in range(2):
        dt_hop(1, h).wait_send()
        dt_hop(2, h).wait_send()
    for kind in range(3):
        for c in range(2):
            di_hop(kind, c).wait_send()
    for cp in final:
        cp.wait()
    for s in range(3):
        for h in range(2):
            dt_hop(s, h).wait_recv()
    for kind in (1, 2):
        for c in range(2):
            di_hop(kind, c).wait_recv()


def score(sc, img_t, txt_t):
    dim = img_t.shape[0]
    any_spec = pl.BlockSpec(memory_space=pl.ANY)
    piece = (dim, HALF)
    hbm = lambda *lead: jax.ShapeDtypeStruct((*lead, *piece), F32)
    dma = lambda k: pltpu.SemaphoreType.DMA((k,))
    flops = 6 * STEPS * BM * 2 * HALF * dim
    return pl.pallas_call(
        kernel,
        name="score",
        out_shape=(jax.ShapeDtypeStruct((4, QR, SN), F32), hbm(8), hbm(2), hbm(3, 2), hbm(2), hbm(2), hbm(2)),
        in_specs=[pl.BlockSpec(memory_space=pltpu.SMEM), any_spec, any_spec],
        out_specs=(pl.BlockSpec(memory_space=pltpu.VMEM),) + (any_spec,) * 6,
        scratch_shapes=[
            pltpu.VMEM((8, BM, dim), BF16),
            pltpu.VMEM((8, dim, BM), BF16),
            pltpu.VMEM((4, 2, dim, HALF), BF16),
            pltpu.VMEM((3, 2, dim, HALF), F32),
            pltpu.VMEM((3, dim, BM), F32),
            pltpu.VMEM((2, BM, SN), F32),
            pltpu.VMEM((2, BM, BN), BF16),
            dma(4), dma(3), dma(3), dma(2), dma(2), dma(2),
            dma(6), dma(6), dma(6), dma(6), dma(6), dma(6), dma(6), dma(6),
        ],
        cost_estimate=pl.CostEstimate(flops=flops, bytes_accessed=2**28, transcendentals=0),
        compiler_params=pltpu.CompilerParams(vmem_limit_bytes=67043328, collective_id=0, has_side_effects=True),
    )(sc, img_t, txt_t)


def embed_t(x, w):
    raw = lax.dot_general(w, x, (((0,), (1,)), ((), ())), preferred_element_type=F32)
    inv = lax.rsqrt(jnp.sum(raw * raw, axis=0, keepdims=True))
    return raw, (raw * inv).astype(BF16)


def tail_kernel(img_sc, txt_sc, st_ref, *refs):
    *ins, out_ref, img_acc, txt_acc = refs
    sums, raws, xs = ins[:3], ins[3], ins[4]
    txt_sums, txt_raw, txt_x = ins[5:9], ins[9], ins[10]
    g = pl.program_id(0)
    dim, img_rows = out_ref.shape[1], xs.shape[1]

    def add_rows(factor, parts, raw_ref, x_ref, acc, start):
        total = parts[0][...].reshape(dim, TAIL)
        for part in parts[1:]:
            total = total + part[...].reshape(dim, TAIL)
        grad = factor[0] * total
        raw = raw_ref[...]
        inv = lax.rsqrt(jnp.sum(raw * raw, axis=0, keepdims=True))
        unit = raw * inv
        raw_grad = inv * (grad - unit * jnp.sum(unit * grad, axis=0, keepdims=True))
        part = dot(raw_grad.astype(BF16), x_ref[...])

        @pl.when(g == start)
        def _():
            acc[...] = part

        @pl.when(g > start)
        def _():
            acc[...] += part

    @pl.when(g < 4)
    def _():
        add_rows(img_sc, sums, raws, xs, img_acc, 0)

    @pl.when(g >= 4)
    def _():
        add_rows(txt_sc, txt_sums, txt_raw, txt_x, txt_acc, 4)

    @pl.when(g == 4)
    def _():
        out_ref[0:img_rows, :] = img_acc[...].T

    @pl.when(g == 7)
    def _():
        last = img_rows + txt_acc.shape[1]
        out_ref[img_rows:last, :] = txt_acc[...].T
        total_rows = txt_sc[1]
        loss = (jnp.sum(st_ref[0]) * LN2 + jnp.sum(st_ref[1])) / total_rows
        d_temp = txt_sc[0] * jnp.sum(st_ref[3])
        d_bias = jnp.sum(st_ref[2]) / total_rows
        row = lax.broadcasted_iota(jnp.int32, (OUT_ROWS - last, dim), 0)
        out_ref[last:OUT_ROWS, :] = jnp.where(row == 0, loss, jnp.where(row == 1, d_temp, d_bias))


def tail(sc, st, di, inc_own, inc_z, img_raw, img_x, dt0, inc_t, txt_raw, txt_x):
    dim = img_raw.shape[0]
    img_f, txt_f = img_x.shape[1], txt_x.shape[1]
    img_g = lambda g: jnp.minimum(g, 3)
    txt_g = lambda g: jnp.maximum(g - 4, 0)
    block = lambda at: pl.BlockSpec((1, dim, TAIL), lambda g: (at(g) // 2, 0, at(g) % 2))
    flat = lambda at: pl.BlockSpec((dim, TAIL), lambda g: (0, at(g)))
    rows = lambda at, f: pl.BlockSpec((TAIL, f), lambda g: (at(g), 0))
    hop = lambda s: pl.BlockSpec((1, 1, dim, TAIL), lambda g: (s, txt_g(g) // 2, 0, txt_g(g) % 2))
    smem = pl.BlockSpec(memory_space=pltpu.SMEM)
    out_rows = OUT_ROWS
    return pl.pallas_call(
        tail_kernel,
        name="tail",
        grid=(8,),
        out_shape=jax.ShapeDtypeStruct((out_rows, dim), F32),
        in_specs=[smem, smem, pl.BlockSpec(st.shape, lambda g: (0, 0, 0)), block(img_g), block(img_g), block(img_g), flat(img_g), rows(img_g, img_f),
                  block(txt_g), hop(0), hop(1), hop(2), flat(txt_g), rows(txt_g, txt_f)],
        out_specs=pl.BlockSpec((out_rows, dim), lambda g: (0, 0)),
        scratch_shapes=[pltpu.VMEM((dim, img_f), F32), pltpu.VMEM((dim, txt_f), F32)],
        compiler_params=pltpu.CompilerParams(vmem_limit_bytes=60 * 2**20, dimension_semantics=("arbitrary",)),
    )(sc, sc, st, di, inc_own, inc_z, img_raw, img_x, dt0, inc_t, inc_t, inc_t, txt_raw, txt_x)


def reduce_kernel(x_ref, img_ref, txt_ref, tot_ref, from_twin, part, got, res, t_send, t_recv, p_send, p_recv, g_send, g_recv, f_send, f_recv, out_sem):
    rep, dat = lax.axis_index("replica"), lax.axis_index("data")
    y, x, core = dat // 4, (dat // 2) % 2, dat % 2

    def flip(bit, on):
        return 1 - bit if on else bit

    def chip(q):
        return flip(rep, q & 4), flip(y, q & 2), flip(x, q & 1)

    def device(q):
        cz, cy, cx = chip(q)
        return (cz, 4 * cy + 2 * cx + core)

    def rows(c, k):
        return pl.ds((2 * c + k) * PART, PART)

    def number(q):
        cz, cy, cx = chip(q)
        return 4 * cz + 2 * cy + cx

    twin = (rep, 4 * y + 2 * x + (1 - core))

    def remote(src, dst, sems, k, to):
        return pltpu.make_async_remote_copy(src_ref=src, dst_ref=dst, send_sem=sems[0].at[k], recv_sem=sems[1].at[k], device_id=to, device_id_type=MESH)

    barrier = pltpu.get_barrier_semaphore()
    for to in [twin] + [device(q) for q in range(1, 8)]:
        pl.semaphore_signal(barrier, inc=1, device_id=to, device_id_type=MESH)
    pl.semaphore_wait(barrier, 8)

    halves = [remote(x_ref.at[rows(c, 1 - core)], from_twin.at[c], (t_send, t_recv), c, twin) for c in range(8)]
    for cp in halves:
        cp.start()
    for c, cp in enumerate(halves):
        cp.wait_recv()
        part[c] = x_ref[rows(c, core), :] + from_twin[c]
    parts = [remote(part.at[number(q)], got.at[q - 1], (p_send, p_recv), q - 1, device(q)) for q in range(1, 8)]
    for cp in parts:
        cp.start()
    total = part[number(0)]
    for q, cp in enumerate(parts):
        cp.wait_recv()
        total = total + got[q]
    mine = rows(number(0), core)
    res[mine, :] = total
    spread = [remote(res.at[mine], res.at[mine], (g_send, g_recv), q - 1, device(q)) for q in range(1, 8)]
    for cp in spread:
        cp.start()
    forward = [remote(res.at[rows(number(q), core)], res.at[rows(number(q), core)], (f_send, f_recv), q, twin) for q in range(8)]
    forward[0].start()
    for q in range(1, 8):
        arrived = res.at[rows(number(q), core)]
        remote(arrived, arrived, (g_send, g_recv), q - 1, device(q)).wait_recv()
        forward[q].start()
    for q in range(8):
        other = res.at[rows(number(q), 1 - core)]
        remote(other, other, (f_send, f_recv), q, twin).wait_recv()
    first, last = img_ref.shape[0], img_ref.shape[0] + txt_ref.shape[0]
    spans = ((img_ref, 0, first), (txt_ref, first, last), (tot_ref, last, last + 8))
    outs = [pltpu.make_async_copy(res.at[pl.ds(lo, hi - lo)], ref, out_sem.at[k]) for k, (ref, lo, hi) in enumerate(spans)]
    for cp in outs:
        cp.start()
    for cp in halves + parts + spread + forward:
        cp.wait_send()
    for cp in outs:
        cp.wait()


def reduce_all(x, img_f, txt_f):
    dim = x.shape[1]
    any_spec = pl.BlockSpec(memory_space=pl.ANY)
    dma = lambda k: pltpu.SemaphoreType.DMA((k,))
    return pl.pallas_call(
        reduce_kernel,
        name="reduce",
        out_shape=tuple(jax.ShapeDtypeStruct((k, dim), F32) for k in (img_f, txt_f, 8)),
        in_specs=[pl.BlockSpec(memory_space=pltpu.VMEM)],
        out_specs=(any_spec,) * 3,
        scratch_shapes=[
            pltpu.VMEM((8, PART, dim), F32),
            pltpu.VMEM((8, PART, dim), F32),
            pltpu.VMEM((7, PART, dim), F32),
            pltpu.VMEM((OUT_ROWS, dim), F32),
            dma(8), dma(8), dma(7), dma(7), dma(7), dma(7), dma(8), dma(8), dma(3),
        ],
        compiler_params=pltpu.CompilerParams(vmem_limit_bytes=40 * 2**20, collective_id=1, has_side_effects=True),
    )(x)


def solution(mesh):
    dev_count = mesh.shape["replica"] * mesh.shape["data"]
    batch_axes = ("replica", "data")

    def local_fn(img_x, txt_x, w_img, w_txt, log_temp, logit_bias):
        total_rows = img_x.shape[0] * dev_count
        img_raw, img_t = embed_t(img_x, w_img)
        txt_raw, txt_t = embed_t(txt_x, w_txt)
        temp_scale = jnp.exp(log_temp[0])
        sc = jnp.stack([temp_scale * LOG2E, logit_bias[0] * LOG2E])
        st, di, dt0, inc_t, _, inc_z, inc_own = score(sc, img_t, txt_t)
        factors = jnp.stack([temp_scale / total_rows, jnp.float32(total_rows)])
        grads = tail(factors, st, di, inc_own, inc_z, img_raw, img_x, dt0, inc_t, txt_raw, txt_x)
        d_w_img, d_w_txt, totals = reduce_all(grads, img_x.shape[1], txt_x.shape[1])
        return totals[0, 0:1], totals[1, 0:1], totals[2, 0:1], d_w_img, d_w_txt

    batch_spec = P(batch_axes, None)
    return jax.shard_map(local_fn, mesh=mesh, in_specs=(batch_spec, batch_spec, P(), P(), P(), P()), out_specs=(P(), P(), P(), P(), P()), check_vma=False)
```
